32 devices in a mesh: batch: 8 (over y, x, core), context: 4 (over z).
Axes of the slice: x: 2, y: 2, z: 4, core: 2. Of those that a mesh axis runs over, the one named last changes fastest.
Arguments:
- hidden: bfloat16 [16, 1024, 1536], P('batch', 'context'), may hold values from -6 to 6
- norm_gain: bfloat16 [1536], P(('batch', 'context')), may hold values from 0.25 to 1.75
- in_weight: bfloat16 [1536, 6448], P(('batch', 'context')), may hold values from -0.15625 to 0.15625
- conv_weight: bfloat16 [4, 3328], P(None, ('batch', 'context')), may hold values from -3 to 3
- conv_bias: bfloat16 [3328], P(('batch', 'context')), may hold values from -1.5 to 1.5
- dt_bias: float32 [48], P('context'), may hold values from -5 to -2
- a_log: float32 [48], P('context'), may hold values from 0 to 2.7
- skip_gain: float32 [48], P('context'), may hold values from 0.5 to 1.5
- gate_gain: bfloat16 [3072], P(('batch', 'context')), may hold values from 0.25 to 1.75
- out_weight: bfloat16 [3072, 1536], P(('batch', 'context')), may hold values from -0.109375 to 0.109375
- cotangent: bfloat16 [16, 1024, 1536], P('batch', 'context'), may hold values from -6 to 6
Outputs:
- output: float32 [16, 1024, 1536], P('batch', 'context')
- grad_hidden: float32 [16, 1024, 1536], P('batch', 'context')
- grad_norm_gain: float32 [1536], P(('batch', 'context'))
- grad_in_weight: float32 [1536, 6448], P(('batch', 'context'))
- grad_conv_weight: float32 [4, 3328], P(None, ('batch', 'context'))
- grad_conv_bias: float32 [3328], P(('batch', 'context'))
- grad_dt_bias: float32 [48], P('context')
- grad_a_log: float32 [48], P('context')
- grad_skip_gain: float32 [48], P('context')
- grad_gate_gain: float32 [3072], P(('batch', 'context'))
- grad_out_weight: float32 [3072, 1536], P(('batch', 'context'))
The draws below stay inside these ranges and needn't reach their ends.
All inputs are finite; a program needn't handle non-finite values.
Results may differ from the reference program's by a relative error of at most 0.012.
Values may be sent and summed in bfloat16 or wider, within the bound.
A program may use at most 256 MiB of HBM per device.

```python
import jax
import jax.numpy as jnp
from jax import lax

D = 1536
DI = 3072
H = 48
N = 128
KW = 4
BLOCK = 256
SEQ_LEN = 1024
SEQ_ALL = 16
EIN = 6448
CONVCH = 3328


def levels(rng, dims, split, least, top_value):
    def one(position, shards_of):
        heights = jax.random.uniform(jax.random.fold_in(jax.random.fold_in(rng, 6), position), (shards_of,), jnp.float32, least / len(split), top_value / len(split))
        return jnp.repeat(jnp.exp(heights), dims[position] // shards_of).reshape((-1,) + (1,) * (len(dims) - position - 1))

    factor_of = one(*split[0])
    for cut in split[1:]:
        factor_of = factor_of * one(*cut)
    return factor_of


def scatter_about(rng, dims, spread, reach, cuts=(), held_as=jnp.bfloat16):
    entries = spread * jax.random.normal(rng, dims, jnp.float32)
    if cuts:
        entries = entries * levels(rng, dims, cuts, -0.22, 0.18)
    return jnp.clip(entries, -reach, reach).astype(held_as)


def setup_inputs(seed: int = 0) -> dict:
    key_list = jax.random.split(jax.random.key(seed), 12)
    return {
        "hidden": scatter_about(key_list[0], (SEQ_ALL, SEQ_LEN, D), 1.0, 6.0, ((0, 8), (1, 4))),
        "norm_gain": jnp.clip(1.0 + 0.15 * jax.random.normal(key_list[1], (D,), jnp.float32), 0.25, 1.75).astype(jnp.bfloat16),
        "in_weight": scatter_about(key_list[2], (D, EIN), D ** -0.5, 0.15625, ((0, 32),)),
        "conv_weight": scatter_about(key_list[3], (KW, CONVCH), KW ** -0.5, 3.0, ((1, 32),)),
        "conv_bias": scatter_about(key_list[4], (CONVCH,), 0.3, 1.5, ((0, 32),)),
        "dt_bias": jnp.clip(-5.0 + 3.0 * jax.random.uniform(key_list[5], (H,), jnp.float32) ** levels(key_list[5], (H,), ((0, 4),), -0.2, 0.2), -5.0, -2.0),
        "a_log": jnp.clip(2.7 * jax.random.uniform(key_list[6], (H,), jnp.float32) ** levels(key_list[6], (H,), ((0, 4),), -0.2, 0.2), 0.0, 2.7),
        "skip_gain": jnp.clip(0.5 + 1.0 * jax.random.uniform(key_list[7], (H,), jnp.float32) ** levels(key_list[7], (H,), ((0, 4),), -0.2, 0.2), 0.5, 1.5),
        "gate_gain": jnp.clip(1.0 + 0.15 * jax.random.normal(key_list[8], (DI,), jnp.float32), 0.25, 1.75).astype(jnp.bfloat16),
        "out_weight": scatter_about(key_list[9], (DI, D), DI ** -0.5, 0.109375, ((0, 32),)),
        "cotangent": scatter_about(key_list[10], (SEQ_ALL, SEQ_LEN, D), 1.0, 6.0, ((0, 8), (1, 4))),
    }


epsilon = 1e-05
highest = lax.Precision.HIGHEST

def rms_scale(values_in, gain):
    factor = lax.rsqrt(lax.optimization_barrier(jnp.mean(values_in * values_in, axis=-1, keepdims=True)) + epsilon)
    return values_in * factor * gain[None, :]

def gated_scale(values_in, gate_rows, gain):
    return rms_scale(values_in * jax.nn.silu(gate_rows), gain)

def causal_conv(values_in, weight, bias):
    length = values_in.shape[0]
    tap_count = weight.shape[0]
    padded = jnp.pad(values_in, ((tap_count - 1, 0), (0, 0)))
    summed = jnp.zeros_like(values_in) + bias[None, :]
    for offset in range(tap_count):
        summed = summed + weight[offset][None, :] * padded[offset:offset + length]
    return jax.nn.silu(summed)

def state_space(inputs, step_sizes, log_rate, b_rows, c_rows, skip_gain):
    length, channels = inputs.shape
    head_count = step_sizes.shape[1]
    head_size = channels // head_count
    blocks = length // BLOCK
    state_dim = b_rows.shape[1]
    x_blocks = inputs.reshape(blocks, BLOCK, head_count, head_size)
    weighted = x_blocks * step_sizes.reshape(blocks, BLOCK, head_count)[..., None]
    log_decay = (step_sizes * (-jnp.exp(log_rate))[None, :]).reshape(blocks, BLOCK, head_count)
    cumulative = jnp.cumsum(log_decay, axis=1)
    b_blocks = b_rows.reshape(blocks, BLOCK, state_dim)
    c_blocks = c_rows.reshape(blocks, BLOCK, state_dim)
    scores = jnp.einsum('cln,csn->cls', c_blocks, b_blocks, precision=highest)
    differ = cumulative[:, :, None, :] - cumulative[:, None, :, :]
    causal = lax.broadcasted_iota(jnp.int32, (BLOCK, BLOCK), 0) >= lax.broadcasted_iota(jnp.int32, (BLOCK, BLOCK), 1)
    decays = jnp.exp(jnp.where(causal[None, :, :, None], differ, -jnp.inf))
    mixing = scores[..., None] * decays
    y_inner = jnp.einsum('clsh,cshp->clhp', mixing, weighted, precision=highest)
    end_decay = jnp.exp(cumulative[:, -1:, :] - cumulative)
    scaled = weighted * end_decay[..., None]
    block_states = jnp.einsum('csn,cshp->chpn', b_blocks, scaled, precision=highest)
    carry_decay = jnp.exp(cumulative[:, -1, :])

    def advance(carried, pieces):
        decay_now, fresh_state = pieces
        return (decay_now[:, None, None] * carried + fresh_state, carried)
    initial = jnp.zeros((head_count, head_size, state_dim), jnp.float32)
    _, previous = lax.scan(advance, initial, (carry_decay, block_states))
    c_scaled = c_blocks[:, :, None, :] * jnp.exp(cumulative)[..., None]
    y_outer = jnp.einsum('clhn,chpn->clhp', c_scaled, previous, precision=highest)
    result = (y_inner + y_outer).reshape(length, channels)
    return result + inputs * jnp.repeat(skip_gain, head_size)[None, :]

def mixer_core(x_pre, bc_pre, dt_pre, conv_x_weight, conv_x_bias, conv_bc_weight, conv_bc_bias, dt_offset, log_rate, skip_gain):
    inputs = causal_conv(x_pre, conv_x_weight, conv_x_bias)
    bc_rows = causal_conv(bc_pre, conv_bc_weight, conv_bc_bias)
    state_dim = bc_rows.shape[1] // 2
    step_sizes = jax.nn.softplus(dt_pre + dt_offset[None, :])
    return state_space(inputs, step_sizes, log_rate, bc_rows[:, :state_dim], bc_rows[:, state_dim:], skip_gain)

def one_sequence(params, hidden_rows, cot_rows):
    norm_gain, in_weight, conv_weight, conv_bias, dt_bias, a_log, skip_gain, gate_gain, out_weight = params
    rows_float = hidden_rows.astype(jnp.float32)
    normed_float, norm_back = jax.vjp(rms_scale, rows_float, norm_gain.astype(jnp.float32))
    normed = normed_float.astype(jnp.bfloat16)
    projected = jnp.dot(normed, in_weight, preferred_element_type=jnp.float32)
    gate_rows = projected[:, :DI]
    x_pre = lax.optimization_barrier(projected[:, DI:2 * DI].astype(jnp.bfloat16))
    bc_pre = lax.optimization_barrier(projected[:, 2 * DI:2 * DI + 2 * N].astype(jnp.bfloat16))
    dt_pre = lax.optimization_barrier(projected[:, 2 * DI + 2 * N:].astype(jnp.bfloat16))
    conv_float = conv_weight.astype(jnp.float32)
    bias_float = conv_bias.astype(jnp.float32)
    mixed, mixer_back = jax.vjp(mixer_core, x_pre.astype(jnp.float32), bc_pre.astype(jnp.float32), dt_pre.astype(jnp.float32), conv_float[:, :DI], bias_float[:DI], conv_float[:, DI:], bias_float[DI:], dt_bias, a_log, skip_gain)
    mixed_round = lax.optimization_barrier(mixed.astype(jnp.bfloat16))
    gated_float, gate_back = jax.vjp(gated_scale, mixed_round.astype(jnp.float32), gate_rows, gate_gain.astype(jnp.float32))
    gated_rows = gated_float.astype(jnp.bfloat16)
    output = rows_float + jnp.dot(gated_rows, out_weight, preferred_element_type=jnp.float32)
    grad_out = jnp.dot(gated_rows.T, cot_rows, preferred_element_type=jnp.float32)
    grad_gated = jnp.dot(cot_rows, out_weight.T, preferred_element_type=jnp.float32)
    grad_mixed, grad_gate, grad_gate_gain = gate_back(grad_gated)
    grad_mixed_round = lax.optimization_barrier(grad_mixed.astype(jnp.bfloat16))
    grads = mixer_back(grad_mixed_round.astype(jnp.float32))
    grad_x_pre, grad_bc_pre, grad_dt_pre, grad_conv_x, grad_bias_x, grad_conv_bc, grad_bias_bc, grad_dt_bias, grad_a_log, grad_skip = grads
    grad_proj = jnp.concatenate([grad_gate.astype(jnp.bfloat16), grad_x_pre.astype(jnp.bfloat16), grad_bc_pre.astype(jnp.bfloat16), grad_dt_pre.astype(jnp.bfloat16)], axis=1)
    grad_in = jnp.dot(normed.T, grad_proj, preferred_element_type=jnp.float32)
    grad_normed = jnp.dot(grad_proj, in_weight.T, preferred_element_type=jnp.float32)
    grad_rows, grad_norm_gain = norm_back(grad_normed)
    grad_hidden = cot_rows.astype(jnp.float32) + grad_rows
    grad_conv = jnp.concatenate([grad_conv_x, grad_conv_bc], axis=1)
    grad_bias = jnp.concatenate([grad_bias_x, grad_bias_bc], axis=0)
    return ((output, grad_hidden), (grad_norm_gain, grad_in, grad_conv, grad_bias, grad_dt_bias, grad_a_log, grad_skip, grad_gate_gain, grad_out))

def add_pair(first_term, second_term):
    return first_term + second_term

def reference(hidden, norm_gain, in_weight, conv_weight, conv_bias, dt_bias, a_log, skip_gain, gate_gain, out_weight, cotangent):
    params = (norm_gain, in_weight, conv_weight, conv_bias, dt_bias, a_log, skip_gain, gate_gain, out_weight)

    def visit(totals, pieces):
        hidden_rows, cot_rows = pieces
        outputs, grads = one_sequence(params, hidden_rows, cot_rows)
        return (jax.tree.map(add_pair, totals, grads), outputs)
    zero_grads = (jnp.zeros((D,), jnp.float32), jnp.zeros((D, EIN), jnp.float32), jnp.zeros((KW, CONVCH), jnp.float32), jnp.zeros((CONVCH,), jnp.float32), jnp.zeros((H,), jnp.float32), jnp.zeros((H,), jnp.float32), jnp.zeros((H,), jnp.float32), jnp.zeros((DI,), jnp.float32), jnp.zeros((DI, D), jnp.float32))
    totals, outputs = lax.scan(visit, zero_grads, (hidden, cotangent))
    return (outputs[0], outputs[1], totals[0], totals[1], totals[2], totals[3], totals[4], totals[5], totals[6], totals[7], totals[8])
```

```python
import functools

import jax
import jax.numpy as jnp
from jax import lax
from jax.experimental import pallas as pl
from jax.experimental.pallas import tpu as pltpu
from jax.sharding import PartitionSpec as P

MESH = pl.DeviceIdType.MESH
epsilon = 1e-05
highest = lax.Precision.HIGHEST
f32 = jnp.float32
bf16 = jnp.bfloat16
GROUP = 512
TILE = 128
HALO = 8
NT = (((1,), (1,)), ((), ()))
TN = (((0,), (0,)), ((), ()))


def dot(a, b, dims=(((1,), (0,)), ((), ()))):
    return lax.dot_general(a, b, dims, preferred_element_type=f32)


def enter(n):
    z = lax.axis_index("context")
    barrier = pltpu.get_barrier_semaphore()

    @pl.when(z > 0)
    def _():
        pl.semaphore_signal(barrier, inc=1, device_id={"context": z - 1}, device_id_type=MESH)

    @pl.when(z < n - 1)
    def _():
        pl.semaphore_signal(barrier, inc=1, device_id={"context": z + 1}, device_id_type=MESH)

    edge = jnp.logical_or(z == 0, z == n - 1)

    @pl.when(edge)
    def _():
        pl.semaphore_wait(barrier, 1)

    @pl.when(jnp.logical_not(edge))
    def _():
        pl.semaphore_wait(barrier, 2)


def conv_act(xp_ref, xh_ref, cw_ref, xs, length):
    taps = 4
    xs[0:HALO, :] = xh_ref[0]
    xs[HALO : HALO + length, :] = xp_ref[0].astype(f32)
    total = cw_ref[taps : taps + 1, :]
    for k in range(taps):
        first = HALO - taps + 1 + k
        total = total + cw_ref[k : k + 1, :] * xs[first : first + length, :]
    sig = jax.nn.sigmoid(total)
    return total, sig, total * sig


def spread(dc_ref, heads, length):
    lane = lax.broadcasted_iota(jnp.int32, (length, 128), 1) < 64
    cols, cums, dts = [], [], []
    for h in range(heads):
        cols.append(jnp.broadcast_to(dc_ref[0, 0, :, heads + h : heads + h + 1], (length, 128)))
    for p in range(heads // 2):
        h = 2 * p
        cums.append(jnp.where(lane, cols[h], cols[h + 1]))
        d0 = jnp.broadcast_to(dc_ref[0, 0, :, h : h + 1], (length, 128))
        d1 = jnp.broadcast_to(dc_ref[0, 0, :, h + 1 : h + 2], (length, 128))
        dts.append(jnp.where(lane, d0, d1))
    return cols, jnp.concatenate(cums, axis=1), jnp.concatenate(dts, axis=1)


def halves(pair):
    lane = lax.broadcasted_iota(jnp.int32, pair.shape, 1) < 64
    zero = jnp.zeros_like(pair)
    return jnp.where(lane, pair, zero), jnp.where(lane, zero, pair)


def forward_kernel(
    n,
    groups,
    steps,
    xp_ref,
    xh_ref,
    cw_ref,
    dc_ref,
    cr_ref,
    b_ref,
    c_ref,
    bt_ref,
    sk_ref,
    y_ref,
    sin_ref,
    xs,
    gmat,
    sent,
    got,
    send_sem,
    recv_sem,
):
    step = pl.program_id(0) * groups + pl.program_id(1)
    z = lax.axis_index("context")
    length = xp_ref.shape[1]
    heads = cr_ref.shape[2]
    tiles = length // TILE

    def handoff(i):
        return pltpu.make_async_remote_copy(
            src_ref=sent.at[i],
            dst_ref=got.at[i],
            send_sem=send_sem.at[i],
            recv_sem=recv_sem.at[i],
            device_id={"context": lax.rem(z + 1, n)},
            device_id_type=MESH,
        )

    @pl.when(step == 0)
    def _():
        enter(n)

    @pl.when(pl.program_id(1) == 0)
    def _():
        gmat[...] = dot(c_ref[0], b_ref[0], NT)

    _, _, x = conv_act(xp_ref, xh_ref, cw_ref, xs, length)
    cols, cumx, dtx = spread(dc_ref, heads, length)
    cend = cumx[length - 1 : length, :]
    weighted = x * dtx
    w16 = weighted.astype(bf16)
    local = dot(bt_ref[0], (weighted * jnp.exp(cend - cumx)).astype(bf16))

    @pl.when(z == 0)
    def _():
        got[step] = jnp.zeros(got.shape[1:], bf16)

    @pl.when(z > 0)
    def _():
        handoff(step).wait_recv()

    state = got[step]
    sin_ref[0] = state

    @pl.when(z < n - 1)
    def _():
        sent[step] = (jnp.exp(cend) * state.astype(f32) + local).astype(bf16)
        handoff(step).start()

    base = jnp.exp(cumx) * dot(c_ref[0], state) + sk_ref[0:1, :] * x
    keep = lax.broadcasted_iota(jnp.int32, (TILE, TILE), 0) >= lax.broadcasted_iota(
        jnp.int32, (TILE, TILE), 1
    )
    for p in range(heads // 2):
        wide = slice(128 * p, 128 * p + 128)
        parts = halves(w16[:, wide])
        for i in range(tiles):
            rows = slice(i * TILE, (i + 1) * TILE)
            left, right = [], []
            for e in range(2):
                h = 2 * p + e
                for j in range(i + 1):
                    across = slice(j * TILE, (j + 1) * TILE)
                    gap = cols[h][rows] - cr_ref[0, 0, h : h + 1, across]
                    if i == j:
                        gap = jnp.where(keep, gap, -1e30)
                    left.append((gmat[rows, across] * jnp.exp(gap)).astype(bf16))
                    right.append(parts[e][across])
            y_ref[0, rows, wide] = base[rows, wide] + dot(
                jnp.concatenate(left, axis=1), jnp.concatenate(right, axis=0)
            )

    @pl.when(jnp.logical_and(step == steps - 1, z < n - 1))
    def _():
        for i in range(steps):
            handoff(i).wait_send()


def gate_kernel(y_ref, gate_ref, gg_ref, gain_ref, gated_ref, gm_ref, ggate_ref, gain_grad_ref):
    @pl.when(pl.program_id(0) == 0)
    def _():
        gain_grad_ref[...] = jnp.zeros_like(gain_grad_ref)

    gate = gate_ref[...]
    sig = jax.nn.sigmoid(gate)
    act = gate * sig
    mixed = y_ref[...].astype(bf16).astype(f32)
    values = mixed * act
    width = values.shape[1]
    factor = lax.rsqrt(jnp.sum(values * values, axis=1, keepdims=True) / width + epsilon)
    scaled = values * factor
    gain = gain_ref[...]
    gated_ref[...] = (scaled * gain).astype(bf16)
    grad = gg_ref[...]
    grad_scaled = grad * gain
    term = grad * scaled
    rows = term.shape[0]
    gain_grad_ref[...] += jnp.sum(term.reshape(rows // 8, 8, width), axis=0)
    mean = jnp.sum(grad_scaled * scaled, axis=1, keepdims=True) / width
    grad_values = factor * (grad_scaled - scaled * mean)
    gm_ref[...] = (grad_values * act).astype(bf16)
    ggate_ref[...] = (grad_values * mixed * (sig * (1.0 + gate * (1.0 - sig)))).astype(bf16)


def backward_kernel(
    n,
    groups,
    steps,
    xp_ref,
    xh_ref,
    cw_ref,
    dc_ref,
    cr_ref,
    b_ref,
    c_ref,
    ct_ref,
    sk_ref,
    y_ref,
    gm_ref,
    sin_ref,
    gx_ref,
    head_ref,
    sums_ref,
    ga_ref,
    gbc_ref,
    xs,
    gas,
    gmat,
    ggmat,
    gb_acc,
    gc_acc,
    sent,
    got,
    send_sem,
    recv_sem,
):
    g = pl.program_id(1)
    step = pl.program_id(0) * groups + g
    z = lax.axis_index("context")
    length = xp_ref.shape[1]
    heads = cr_ref.shape[2]
    tiles = length // TILE
    state_dim = b_ref.shape[2]

    def handoff(i):
        return pltpu.make_async_remote_copy(
            src_ref=sent.at[i],
            dst_ref=got.at[i],
            send_sem=send_sem.at[i],
            recv_sem=recv_sem.at[i],
            device_id={"context": lax.rem(z + n - 1, n)},
            device_id_type=MESH,
        )

    @pl.when(step == 0)
    def _():
        enter(n)

    @pl.when(g == 0)
    def _():
        gmat[...] = dot(b_ref[0], c_ref[0], NT)
        ggmat[...] = jnp.zeros_like(ggmat)
        gb_acc[...] = jnp.zeros_like(gb_acc)
        gc_acc[...] = jnp.zeros_like(gc_acc)

    cols, cumx, dtx = spread(dc_ref, heads, length)
    cend = cumx[length - 1 : length, :]
    gm = gm_ref[0]
    gy = gm.astype(f32)
    faded = (jnp.exp(cumx) * gy).astype(bf16)
    local = dot(ct_ref[0], faded)

    @pl.when(z == n - 1)
    def _():
        got[step] = jnp.zeros(got.shape[1:], bf16)

    @pl.when(z < n - 1)
    def _():
        handoff(step).wait_recv()

    gstate = got[step]

    @pl.when(z > 0)
    def _():
        sent[step] = (jnp.exp(cend) * gstate.astype(f32) + local).astype(bf16)
        handoff(step).start()

    pre, sig, x = conv_act(xp_ref, xh_ref, cw_ref, xs, length)
    weighted = x * dtx
    w16 = weighted.astype(bf16)
    tail = jnp.exp(cend - cumx)
    gw_state = tail * dot(b_ref[0], gstate)
    state = sin_ref[0]
    gc_acc[...] += dot(faded, state, NT)
    gb_acc[...] += dot((tail * weighted).astype(bf16), gstate, NT)
    keep = lax.broadcasted_iota(jnp.int32, (TILE, TILE), 0) <= lax.broadcasted_iota(
        jnp.int32, (TILE, TILE), 1
    )
    grids = {}
    pairs = []
    for p in range(heads // 2):
        wide = slice(128 * p, 128 * p + 128)
        parts = halves(gm[:, wide])
        w_parts = halves(w16[:, wide])
        gm_pair = gm[:, wide]
        rows_out = []
        for i in range(tiles):
            rows = slice(i * TILE, (i + 1) * TILE)
            left, right = [], []
            for e in range(2):
                h = 2 * p + e
                for j in range(i, tiles):
                    across = slice(j * TILE, (j + 1) * TILE)
                    gap = cr_ref[0, 0, h : h + 1, across] - cols[h][rows]
                    if i == j:
                        gap = jnp.where(keep, gap, -1e30)
                    decay = jnp.exp(gap)
                    left.append((gmat[rows, across] * decay).astype(bf16))
                    right.append(parts[e][across])
                    product = dot(w_parts[e][rows], gm_pair[across], NT) * decay
                    grids[i, j] = grids[i, j] + product if (i, j) in grids else product
            rows_out.append(dot(jnp.concatenate(left, axis=1), jnp.concatenate(right, axis=0)))
        pairs.append(jnp.concatenate(rows_out, axis=0))
    for i, j in grids:
        ggmat[i * TILE : (i + 1) * TILE, j * TILE : (j + 1) * TILE] += grids[i, j]
    gw_inner = jnp.concatenate(pairs, axis=1)
    gw = gw_inner + gw_state
    skip = sk_ref[0:1, :]
    gx = skip * gy + dtx * gw
    first = gy * (y_ref[0] - skip * x) - w16.astype(f32) * gw_inner
    second = weighted * gw_state
    third = x * gw
    width = gm.shape[1]
    chan = lax.broadcasted_iota(jnp.int32, (width, 128), 0) // 64
    lane = lax.broadcasted_iota(jnp.int32, (width, 128), 1)
    total = None
    for which, value in enumerate((first, second, third)):
        pick = (lane == chan + which * heads).astype(bf16)
        high = value.astype(bf16)
        low = (value - high.astype(f32)).astype(bf16)
        piece = dot(high, pick) + dot(low, pick)
        total = piece if total is None else total + piece
    head_ref[0, 0] = total
    ga = gx * (sig * (1.0 + pre * (1.0 - sig)))
    gas[0:length, :] = ga
    gas[length : length + HALO, :] = jnp.zeros((HALO, width), f32)
    ga_ref[0] = ga[0:HALO]
    taps = 4
    out = None
    sums = []
    for k in range(taps):
        piece = cw_ref[k : k + 1, :] * gas[taps - 1 - k : taps - 1 - k + length, :]
        out = piece if out is None else out + piece
        start = HALO - taps + 1 + k
        sums.append(jnp.sum(ga * xs[start : start + length, :], axis=0, keepdims=True))
    gx_ref[0] = out.astype(bf16)
    sums.append(jnp.sum(ga, axis=0, keepdims=True))
    sums.append(jnp.sum(gy * x, axis=0, keepdims=True))
    sums.append(
        jnp.exp(cend) * jnp.sum(state.astype(f32) * gstate.astype(f32), axis=0, keepdims=True)
    )
    sums.append(jnp.zeros((1, width), f32))
    sums_ref[0] = jnp.concatenate(sums, axis=0)

    @pl.when(g == groups - 1)
    def _():
        for i in range(tiles):
            rows = slice(i * TILE, (i + 1) * TILE)
            gb, gc = gb_acc[rows, :], gc_acc[rows, :]
            for j in range(tiles):
                across = slice(j * TILE, (j + 1) * TILE)
                if j >= i:
                    gb += dot(ggmat[rows, across].astype(bf16), c_ref[0, across, :])
                if j <= i:
                    gc += dot(ggmat[across, rows].astype(bf16), b_ref[0, across, :], TN)
            gbc_ref[0, rows, 0:state_dim] = gb
            gbc_ref[0, rows, state_dim : 2 * state_dim] = gc

    @pl.when(jnp.logical_and(step == steps - 1, z > 0))
    def _():
        for i in range(steps):
            handoff(i).wait_send()


def gather_small(parts, axes, rank_of):
    packed = jnp.concatenate([piece.reshape(-1) for piece in parts])
    return lax.all_gather(packed, axes, axis=0, tiled=False)


def body(
    hidden,
    norm_gain,
    in_weight,
    conv_weight,
    conv_bias,
    dt_bias,
    a_log,
    skip_gain,
    gate_gain,
    out_weight,
    cotangent,
):
    axes = ("batch", "context")
    n = lax.axis_size("context")
    devices = n * lax.axis_size("batch")
    z = lax.axis_index("context")
    seqs, length, model = hidden.shape
    inner = gate_gain.shape[0] * devices
    head_count = dt_bias.shape[0] * n
    taps = conv_weight.shape[0]
    ein = in_weight.shape[1]
    states = (ein - 2 * inner - head_count) // 2
    head_size = inner // head_count
    group = GROUP
    groups = inner // group
    heads = group // head_size
    steps = seqs * groups
    tokens = seqs * length

    small = jnp.concatenate(
        [norm_gain, conv_weight.reshape(-1), conv_bias, gate_gain]
    )
    small_all = lax.all_gather(small, axes, axis=0, tiled=False)
    k0 = norm_gain.shape[0]
    kc = conv_bias.shape[0]
    k1 = k0 + taps * kc
    k2 = k1 + kc
    full_norm = small_all[:, :k0].reshape(-1).astype(f32)
    full_conv = (
        small_all[:, k0:k1].reshape(devices, taps, kc).transpose(1, 0, 2).reshape(taps, -1)
    ).astype(f32)
    full_bias = small_all[:, k1:k2].reshape(-1).astype(f32)
    full_gate = small_all[:, k2:].reshape(-1).astype(f32)
    head_params = lax.all_gather(
        jnp.stack([dt_bias, a_log, skip_gain]), "context", axis=1, tiled=True
    )
    w_rest = lax.all_gather(in_weight[:, inner:], axes, axis=0, tiled=True)
    w_gate = lax.all_gather(in_weight[:, :inner], axes, axis=0, tiled=True)
    w_out = lax.all_gather(out_weight, axes, axis=0, tiled=True)

    rows = hidden.reshape(tokens, model).astype(f32)
    factor = lax.rsqrt(jnp.mean(rows * rows, axis=-1, keepdims=True) + epsilon)
    normed = (rows * factor * full_norm[None, :]).astype(bf16)
    proj = dot(normed, w_rest).astype(bf16).reshape(seqs, length, -1)
    gate_rows = dot(normed, w_gate)
    cot_rows = cotangent.reshape(tokens, model)
    grad_gated = dot(cot_rows, w_out, NT)

    up = [(i, i + 1) for i in range(n - 1)]
    down = [(i + 1, i) for i in range(n - 1)]
    halo = lax.ppermute(proj[:, length - HALO :, : inner + 2 * states], "context", up).astype(f32)
    bc_pre = proj[:, :, inner : inner + 2 * states].astype(f32)
    bc_ext = jnp.concatenate([halo[:, HALO - taps + 1 :, inner:], bc_pre], axis=1)
    bc_act = full_bias[inner:] + sum(
        full_conv[k, inner:] * bc_ext[:, k : k + length] for k in range(taps)
    )
    bc_sig = jax.nn.sigmoid(bc_act)
    bc16 = (bc_act * bc_sig).astype(bf16)
    b16, c16 = bc16[..., :states], bc16[..., states:]
    bt16, ct16 = b16.transpose(0, 2, 1), c16.transpose(0, 2, 1)

    full_dt, full_log, full_skip = head_params[0], head_params[1], head_params[2]
    rate = -jnp.exp(full_log)
    dt_in = proj[:, :, inner + 2 * states :].astype(f32) + full_dt
    dt = jax.nn.softplus(dt_in)
    lower = (
        lax.broadcasted_iota(jnp.int32, (length, length), 0)
        >= lax.broadcasted_iota(jnp.int32, (length, length), 1)
    ).astype(f32)
    log_decay = dt * rate
    cum = jnp.einsum("ts,qsh->qth", lower, log_decay, precision=highest)

    def grouped(value):
        return value.reshape(seqs, length, groups, heads).transpose(0, 2, 1, 3)

    dt_cum = jnp.concatenate([grouped(dt), grouped(cum)], axis=-1)
    cum_rows = cum.transpose(0, 2, 1).reshape(seqs, groups, heads, length)
    skip_row = jnp.broadcast_to(jnp.repeat(full_skip, head_size)[None, :], (8, inner))
    conv_rows = jnp.concatenate(
        [full_conv[:, :inner], full_bias[None, :inner], jnp.zeros((3, inner), f32)], axis=0
    )
    halo_x = halo[:, :, :inner]

    seq_block = lambda q, g: (q, 0, g)
    whole = lambda q, g: (q, 0, 0)
    four = lambda q, g: (q, g, 0, 0)
    param = lambda q, g: (0, g)
    common = [
        pl.BlockSpec((1, length, group), seq_block),
        pl.BlockSpec((1, HALO, group), seq_block),
        pl.BlockSpec((8, group), param),
        pl.BlockSpec((1, 1, length, 2 * heads), four),
        pl.BlockSpec((1, 1, heads, length), four),
        pl.BlockSpec((1, length, states), whole),
        pl.BlockSpec((1, length, states), whole),
        pl.BlockSpec((1, states, length), whole),
        pl.BlockSpec((8, group), param),
    ]
    y, s_in = pl.pallas_call(
        functools.partial(forward_kernel, n, groups, steps),
        grid=(seqs, groups),
        in_specs=common,
        out_specs=[
            pl.BlockSpec((1, length, group), seq_block),
            pl.BlockSpec((1, states, group), seq_block),
        ],
        out_shape=[
            jax.ShapeDtypeStruct((seqs, length, inner), f32),
            jax.ShapeDtypeStruct((seqs, states, inner), bf16),
        ],
        scratch_shapes=[
            pltpu.VMEM((length + HALO, group), f32),
            pltpu.VMEM((length, length), f32),
            pltpu.VMEM((steps, states, group), bf16),
            pltpu.VMEM((steps, states, group), bf16),
            pltpu.SemaphoreType.DMA((steps,)),
            pltpu.SemaphoreType.DMA((steps,)),
        ],
        compiler_params=pltpu.CompilerParams(
            collective_id=1,
            has_side_effects=True,
            dimension_semantics=("arbitrary", "arbitrary"),
            vmem_limit_bytes=40 << 20,
        ),
        cost_estimate=pl.CostEstimate(
            flops=8 * tokens * inner * 512, bytes_accessed=tokens * inner * 8, transcendentals=0
        ),
        name="mixer_forward",
    )(proj, halo_x, conv_rows, dt_cum, cum_rows, b16, c16, bt16, skip_row)

    tile_rows = 64
    row_spec = pl.BlockSpec((tile_rows, inner), lambda i: (i, 0))
    gated, grad_mixed, grad_gate, gain_grad = pl.pallas_call(
        gate_kernel,
        grid=(tokens // tile_rows,),
        in_specs=[row_spec, row_spec, row_spec, pl.BlockSpec((1, inner), lambda i: (0, 0))],
        out_specs=[row_spec, row_spec, row_spec, pl.BlockSpec((8, inner), lambda i: (0, 0))],
        out_shape=[
            jax.ShapeDtypeStruct((tokens, inner), bf16),
            jax.ShapeDtypeStruct((tokens, inner), bf16),
            jax.ShapeDtypeStruct((tokens, inner), bf16),
            jax.ShapeDtypeStruct((8, inner), f32),
        ],
        compiler_params=pltpu.CompilerParams(
            dimension_semantics=("arbitrary",), vmem_limit_bytes=40 << 20
        ),
        cost_estimate=pl.CostEstimate(
            flops=tokens * inner * 40, bytes_accessed=tokens * inner * 18, transcendentals=0
        ),
        name="gate_both",
    )(y.reshape(tokens, inner), gate_rows, grad_gated, full_gate[None, :])

    output = rows + dot(gated, w_out)
    grad_out = dot(gated, cot_rows, TN).astype(bf16)
    share_out = lax.psum_scatter(grad_out, axes, scatter_dimension=0, tiled=True).astype(f32)
    grad_in_gate = dot(normed, grad_gate, TN).astype(bf16)
    share_gate = lax.psum_scatter(grad_in_gate, axes, scatter_dimension=0, tiled=True).astype(f32)

    gx, head_sums, sums, ga_first, gbc = pl.pallas_call(
        functools.partial(backward_kernel, n, groups, steps),
        grid=(seqs, groups),
        in_specs=common
        + [
            pl.BlockSpec((1, length, group), seq_block),
            pl.BlockSpec((1, length, group), seq_block),
            pl.BlockSpec((1, states, group), seq_block),
        ],
        out_specs=[
            pl.BlockSpec((1, length, group), seq_block),
            pl.BlockSpec((1, 1, length, 128), four),
            pl.BlockSpec((1, 8, group), seq_block),
            pl.BlockSpec((1, HALO, group), seq_block),
            pl.BlockSpec((1, length, 2 * states), whole),
        ],
        out_shape=[
            jax.ShapeDtypeStruct((seqs, length, inner), bf16),
            jax.ShapeDtypeStruct((seqs, groups, length, 128), f32),
            jax.ShapeDtypeStruct((seqs, 8, inner), f32),
            jax.ShapeDtypeStruct((seqs, HALO, inner), f32),
            jax.ShapeDtypeStruct((seqs, length, 2 * states), f32),
        ],
        scratch_shapes=[
            pltpu.VMEM((length + HALO, group), f32),
            pltpu.VMEM((length + HALO, group), f32),
            pltpu.VMEM((length, length), f32),
            pltpu.VMEM((length, length), f32),
            pltpu.VMEM((length, states), f32),
            pltpu.VMEM((length, states), f32),
            pltpu.VMEM((steps, states, group), bf16),
            pltpu.VMEM((steps, states, group), bf16),
            pltpu.SemaphoreType.DMA((steps,)),
            pltpu.SemaphoreType.DMA((steps,)),
        ],
        compiler_params=pltpu.CompilerParams(
            collective_id=2,
            has_side_effects=True,
            dimension_semantics=("arbitrary", "arbitrary"),
            vmem_limit_bytes=48 << 20,
        ),
        cost_estimate=pl.CostEstimate(
            flops=16 * tokens * inner * 512, bytes_accessed=tokens * inner * 12, transcendentals=0
        ),
        name="mixer_backward",
    )(
        proj,
        halo_x,
        conv_rows,
        dt_cum,
        cum_rows,
        b16,
        c16,
        ct16,
        skip_row,
        y,
        grad_mixed.reshape(seqs, length, inner),
        s_in,
    )

    ga_bc = gbc * (bc_sig * (1.0 + bc_act * (1.0 - bc_sig)))
    ga_next = lax.ppermute(
        jnp.concatenate([ga_first, ga_bc[:, :HALO]], axis=-1), "context", down
    )
    bc_gext = jnp.concatenate([ga_bc, ga_next[:, : taps - 1, inner:]], axis=1)
    grad_bc = sum(
        full_conv[k, inner:] * bc_gext[:, taps - 1 - k : taps - 1 - k + length]
        for k in range(taps)
    )
    grad_conv_bc = jnp.stack(
        [jnp.sum(ga_bc * bc_ext[:, k : k + length], axis=(0, 1)) for k in range(taps)]
    )
    grad_bias_bc = jnp.sum(ga_bc, axis=(0, 1))
    edge_ext = jnp.concatenate(
        [jnp.zeros((seqs, HALO, inner), f32), ga_next[:, :, :inner]], axis=1
    )
    edge = sum(
        full_conv[k, :inner] * edge_ext[:, taps - 1 - k : taps - 1 - k + HALO]
        for k in range(taps)
    )
    gx_last = (gx[:, length - HALO :].astype(f32) + edge).astype(bf16)
    grad_x = jnp.concatenate([gx[:, : length - HALO], gx_last], axis=1)

    def ungrouped(which):
        piece = head_sums[..., which * heads : (which + 1) * heads]
        return piece.transpose(0, 2, 1, 3).reshape(seqs, length, head_count)

    per_head = jnp.sum(
        sums[:, 5:7].reshape(seqs, 2, head_count, head_size), axis=-1
    )
    strict = lower - jnp.eye(length, dtype=f32)
    grad_log = (
        jnp.einsum("lt,qlh->qth", lower, ungrouped(0), precision=highest)
        + jnp.einsum("ts,qsh->qth", strict, ungrouped(1), precision=highest)
        + per_head[:, 1][:, None, :]
    )
    grad_dt = ungrouped(2) + grad_log * rate
    grad_dt_in = grad_dt * jax.nn.sigmoid(dt_in)
    grad_dt_bias = jnp.sum(grad_dt_in, axis=(0, 1))
    grad_a_log = jnp.sum(grad_log * log_decay, axis=(0, 1))
    grad_skip = jnp.sum(per_head[:, 0], axis=0)

    grad_rest = jnp.concatenate(
        [grad_x, grad_bc.astype(bf16), grad_dt_in.astype(bf16)], axis=-1
    ).reshape(tokens, -1)
    grad_in_rest = dot(normed, grad_rest, TN).astype(bf16)
    share_rest = lax.psum_scatter(grad_in_rest, axes, scatter_dimension=0, tiled=True).astype(f32)
    grad_normed = dot(grad_gate, w_gate, NT) + dot(grad_rest, w_rest, NT)
    scaled = rows * factor
    grad_norm = jnp.sum(grad_normed * scaled, axis=0)
    grad_scaled = grad_normed * full_norm[None, :]
    grad_rows = factor * (
        grad_scaled - scaled * jnp.mean(grad_scaled * scaled, axis=-1, keepdims=True)
    )
    grad_hidden = cot_rows.astype(f32) + grad_rows

    grad_conv = jnp.concatenate([jnp.sum(sums[:, :taps], axis=0), grad_conv_bc], axis=1)
    grad_bias = jnp.concatenate([jnp.sum(sums[:, 4], axis=0), grad_bias_bc], axis=0)
    grad_gain = jnp.sum(gain_grad, axis=0)
    heads_all = jnp.broadcast_to(
        jnp.stack([grad_dt_bias, grad_a_log, grad_skip])
        .reshape(3, n, -1)
        .transpose(1, 0, 2)
        .reshape(1, n, -1),
        (devices // n, n, 3 * head_count // n),
    ).reshape(devices, -1)
    packed = jnp.concatenate(
        [
            grad_norm.reshape(devices, -1),
            grad_conv.reshape(taps, devices, -1).transpose(1, 0, 2).reshape(devices, -1),
            grad_bias.reshape(devices, -1),
            grad_gain.reshape(devices, -1),
            heads_all,
        ],
        axis=1,
    )
    mine = lax.psum_scatter(packed, axes, scatter_dimension=0, tiled=False)
    k3 = k2 + gate_gain.shape[0]
    kh = dt_bias.shape[0]
    share_in = jnp.concatenate([share_gate, share_rest], axis=1)
    return (
        output.reshape(seqs, length, model),
        grad_hidden.reshape(seqs, length, model),
        mine[:k0],
        share_in,
        mine[k0:k1].reshape(taps, kc),
        mine[k1:k2],
        mine[k3 : k3 + kh],
        mine[k3 + kh : k3 + 2 * kh],
        mine[k3 + 2 * kh :],
        mine[k2:k3],
        share_out,
    )


def solution(mesh):
    in_specs = (
        P("batch", "context", None),
        P(("batch", "context")),
        P(("batch", "context"), None),
        P(None, ("batch", "context")),
        P(("batch", "context")),
        P("context"),
        P("context"),
        P("context"),
        P(("batch", "context")),
        P(("batch", "context"), None),
        P("batch", "context", None),
    )
    out_specs = (
        P("batch", "context", None),
        P("batch", "context", None),
        P(("batch", "context")),
        P(("batch", "context"), None),
        P(None, ("batch", "context")),
        P(("batch", "context")),
        P("context"),
        P("context"),
        P("context"),
        P(("batch", "context")),
        P(("batch", "context"), None),
    )
    return jax.shard_map(body, mesh=mesh, in_specs=in_specs, out_specs=out_specs, check_vma=False)
```
